32 devices in a mesh: dp: 1 (over z), sp: 32 (over y, x, core).
Axes of the slice: x: 4, y: 4, z: 1, core: 2. Of those that a mesh axis runs over, the one named last changes fastest.
The devices are a block of a 4x4x8 slice.
Arguments:
- x: bfloat16 [16, 1024, 256], P('dp', 'sp')
- w_cur: bfloat16 [16, 8, 256, 512], replicated
- w_past: bfloat16 [16, 8, 256, 512], replicated
- w_res: bfloat16 [16, 8, 256, 256], replicated
- w_skip: bfloat16 [16, 8, 256, 256], replicated
Outputs:
- output 1: float32 [16, 32, 32, 256], P('dp', 'sp')
- output 2: float32 [16, 32, 32, 256], P('dp', 'sp')
All inputs are finite; a program needn't handle non-finite values.
Results may differ from the reference program's by a relative error of at most 0.0089469.
Values are sent between devices in bfloat16 or wider.
A program may use at most 768 MiB of HBM per device.

```python
import jax
import jax.numpy as jnp
from jax import lax

BATCH_PART = 16
SEQ_DEV = 32
GROUP_SIZE = 32
STACKS = 16
CHANNELS = 256
SKIP_CH = 256
CYCLE_LEN = 8

SEQ_LEN = SEQ_DEV * GROUP_SIZE
LAYERS = STACKS * CYCLE_LEN


def setup_inputs(seed: int = 0, part: int = 0) -> dict:
    base_key = jax.random.key(seed)
    key_x = jax.random.fold_in(jax.random.fold_in(base_key, 1), part)
    key_w = jax.random.split(jax.random.fold_in(base_key, 2), 4)
    tap_scale = (2 * CHANNELS) ** -0.5
    out_scale = 2.0 * (CHANNELS * LAYERS) ** -0.5
    tap_shape = (STACKS, CYCLE_LEN, CHANNELS, 2 * CHANNELS)
    x = jax.random.normal(key_x, (BATCH_PART, SEQ_LEN, CHANNELS), jnp.float32)
    w_cur = jax.random.normal(key_w[0], tap_shape, jnp.float32) * tap_scale
    w_past = jax.random.normal(key_w[1], tap_shape, jnp.float32) * tap_scale
    w_res = jax.random.normal(key_w[2], (STACKS, CYCLE_LEN, CHANNELS, CHANNELS), jnp.float32) * out_scale
    w_skip = jax.random.normal(key_w[3], (STACKS, CYCLE_LEN, CHANNELS, SKIP_CH), jnp.float32) * out_scale
    return {"x": x.astype(jnp.bfloat16), "w_cur": w_cur.astype(jnp.bfloat16), "w_past": w_past.astype(jnp.bfloat16), "w_res": w_res.astype(jnp.bfloat16), "w_skip": w_skip.astype(jnp.bfloat16)}


def gated_layer(h_res, skip_acc, cur_w, past_w, res_w, skip_w, dilation):
    row_count = BATCH_PART * SEQ_LEN
    u_cur = h_res.astype(jnp.bfloat16)
    u_past = jnp.concatenate([jnp.zeros((BATCH_PART, dilation, CHANNELS), jnp.bfloat16), u_cur[:, :SEQ_LEN - dilation]], axis=1)
    pre_act = jnp.dot(u_cur.reshape(row_count, CHANNELS), cur_w, preferred_element_type=jnp.float32) + jnp.dot(u_past.reshape(row_count, CHANNELS), past_w, preferred_element_type=jnp.float32)
    gated = (jnp.tanh(pre_act[:, :CHANNELS]) * jax.nn.sigmoid(pre_act[:, CHANNELS:])).astype(jnp.bfloat16)
    h_new = h_res + jnp.dot(gated, res_w, preferred_element_type=jnp.float32).reshape(BATCH_PART, SEQ_LEN, CHANNELS)
    skip_new = skip_acc + jnp.dot(gated, skip_w, preferred_element_type=jnp.float32).reshape(BATCH_PART, SEQ_LEN, SKIP_CH)
    return h_new, skip_new


def reference(x, w_cur, w_past, w_res, w_skip):
    def stack_body(carry, weights):
        h_res, skip_acc = carry
        stack_cur, stack_past, stack_res, stack_skip = weights
        for layer_pos in range(CYCLE_LEN):
            h_res, skip_acc = gated_layer(h_res, skip_acc, stack_cur[layer_pos], stack_past[layer_pos], stack_res[layer_pos], stack_skip[layer_pos], 2 ** layer_pos)
        return (h_res, skip_acc), None

    h_start = x.astype(jnp.float32)
    skip_start = jnp.zeros((BATCH_PART, SEQ_LEN, SKIP_CH), jnp.float32)
    (h_fin, skip_fin), unused = lax.scan(stack_body, (h_start, skip_start), (w_cur, w_past, w_res, w_skip))
    h_out = h_fin.reshape(BATCH_PART, SEQ_DEV, GROUP_SIZE, CHANNELS).transpose(0, 2, 1, 3)
    skip_out = skip_fin.reshape(BATCH_PART, SEQ_DEV, GROUP_SIZE, SKIP_CH).transpose(0, 2, 1, 3)
    return (h_out, skip_out)
```

```python
import functools

import jax
import jax.numpy as jnp
from jax import lax
from jax.experimental import pallas as pl
from jax.experimental.pallas import tpu as pltpu
from jax.sharding import PartitionSpec as P

F32, BF16 = jnp.float32, jnp.bfloat16
LANES = 128


def load_rows(ref, start, count):
    return jnp.concatenate([ref[g, pl.ds(start, count), :] for g in range(ref.shape[0])], axis=1)


def store_rows(ref, start, value):
    for g in range(ref.shape[0]):
        ref[g, pl.ds(start, value.shape[0]), :] = value[:, g * LANES:(g + 1) * LANES]


def gated(z):
    c = z.shape[1] // 2
    return (jnp.tanh(z[:, :c]) * (0.5 * jnp.tanh(0.5 * z[:, c:]) + 0.5)).astype(BF16)


def stack_kernel(n, x_ref, wc, wp, wr, ws, out_ref, xbuf, h, skip, win, wout, halo_out, halo_in, stage,
                 w_sem, x_send, x_recv, halo_send, halo_recv, o_send, o_recv, self_sem):
    me = lax.axis_index("sp")
    batch, seq_dev = x_ref.shape[0], x_ref.shape[1]
    parts = n // batch
    srcs = n // parts
    rows = seq_dev * srcs
    stacks, cycle = wc.shape[0], wc.shape[1]
    reach = 2 ** (cycle - 1)
    seq, part = me // parts, lax.rem(me, parts)
    my_part = me // srcs

    def weight_copies(s, slot):
        return [pltpu.make_async_copy(w.at[s], buf.at[slot, t], w_sem.at[slot, 2 * o + t])
                for o, (buf, pair) in enumerate(((win, (wc, wp)), (wout, (wr, ws)))) for t, w in enumerate(pair)]

    for c in weight_copies(0, 0):
        c.start()
    halo_in[0] = jnp.zeros(halo_in.shape[1:], F32)
    skip[...] = jnp.zeros_like(skip)

    barrier = pltpu.get_barrier_semaphore()

    def greet(k, _):
        pl.semaphore_signal(barrier, inc=1, device_id={"sp": lax.rem(me + k, n)}, device_id_type=pl.DeviceIdType.MESH)
        return 0
    lax.fori_loop(1, n, greet, 0)
    pl.semaphore_wait(barrier, n - 1)

    slot_x = pl.ds(lax.rem(me, srcs) * seq_dev, seq_dev)

    def x_copy(b):
        return pltpu.make_async_remote_copy(
            src_ref=x_ref.at[b], dst_ref=xbuf.at[slot_x], send_sem=x_send.at[b], recv_sem=x_recv.at[lax.rem(me, srcs)],
            device_id={"sp": b * parts + my_part}, device_id_type=pl.DeviceIdType.MESH)

    def x_start(b, _):
        @pl.when(b * parts + my_part != me)
        def _():
            x_copy(b).start()

        @pl.when(b * parts + my_part == me)
        def _():
            pltpu.make_async_copy(x_ref.at[b], xbuf.at[slot_x], x_recv.at[lax.rem(me, srcs)]).start()
        return 0
    lax.fori_loop(0, batch, x_start, 0)

    def x_wait(i, _):
        pltpu.make_async_copy(x_ref.at[0], xbuf.at[pl.ds(i * seq_dev, seq_dev)], x_recv.at[i]).wait()
        return 0
    lax.fori_loop(0, srcs, x_wait, 0)
    store_rows(h.at[0], reach, xbuf[...].astype(F32))

    def layer(s, i, slot):
        src, dst = h.at[i % 2], h.at[(i + 1) % 2]
        d = 2 ** i
        for g in range(h.shape[1]):
            src[g, pl.ds(reach - d, d), :] = halo_in[s * part, g, pl.ds(d, d), :]
            halo_out[s, g, pl.ds(d, d), :] = src[g, pl.ds(reach + rows - d, d), :]
        cur = load_rows(src, reach, rows)
        past = load_rows(src, reach - d, rows).astype(BF16)
        z = (jnp.dot(cur.astype(BF16), win[slot, 0, i], preferred_element_type=F32)
             + jnp.dot(past, win[slot, 1, i], preferred_element_type=F32))
        a = gated(z)
        store_rows(dst, reach, cur + jnp.dot(a, wout[slot, 0, i], preferred_element_type=F32))
        store_rows(skip, 0, load_rows(skip, 0, rows) + jnp.dot(a, wout[slot, 1, i], preferred_element_type=F32))

    def halo_copy(s):
        return pltpu.make_async_remote_copy(
            src_ref=halo_out.at[s], dst_ref=halo_in.at[s], send_sem=halo_send.at[s], recv_sem=halo_recv.at[s],
            device_id={"sp": jnp.minimum(me + 1, n - 1)}, device_id_type=pl.DeviceIdType.MESH)

    def stack(s, _):
        slot = lax.rem(s, 2)
        for c in weight_copies(s, slot):
            c.wait()

        @pl.when(s + 1 < stacks)
        def _():
            for c in weight_copies(s + 1, 1 - slot):
                c.start()

        @pl.when(part > 0)
        def _():
            halo_copy(s).wait_recv()
        for i in range(cycle):
            layer(s, i, slot)

        @pl.when(part < parts - 1)
        def _():
            halo_copy(s).start()
        return 0
    lax.fori_loop(0, stacks, stack, 0)

    per = rows // n
    for j in range(n):
        for g in range(h.shape[1]):
            stage[j, 0, :, g * LANES:(g + 1) * LANES] = h[0, g, pl.ds(reach + j, per, stride=n), :]
            stage[j, 1, :, g * LANES:(g + 1) * LANES] = skip[g, pl.ds(j, per, stride=n), :]

    def out_copy(target, source):
        return pltpu.make_async_remote_copy(
            src_ref=stage.at[target], dst_ref=out_ref.at[source // parts, lax.rem(source, parts)],
            send_sem=o_send.at[target], recv_sem=o_recv.at[source],
            device_id={"sp": target}, device_id_type=pl.DeviceIdType.MESH)

    def out_start(k, _):
        out_copy(lax.rem(me + k, n), me).start()
        return 0
    lax.fori_loop(1, n, out_start, 0)
    own = pltpu.make_async_copy(stage.at[me], out_ref.at[seq, part], self_sem)
    own.start()

    def out_wait(k, _):
        other = lax.rem(me + k, n)
        out_copy(other, other).wait()
        return 0
    lax.fori_loop(1, n, out_wait, 0)
    own.wait()

    def x_done(b, _):
        @pl.when(b * parts + my_part != me)
        def _():
            x_copy(b).wait_send()
        return 0
    lax.fori_loop(0, batch, x_done, 0)

    @pl.when(part < parts - 1)
    def _():
        def sent(s, _):
            halo_copy(s).wait_send()
            return 0
        lax.fori_loop(0, stacks, sent, 0)


def solution(mesh):
    n = mesh.shape["sp"]

    def local_stack(x_loc, w_cur, w_past, w_res, w_skip):
        batch, seq_dev, channels = x_loc.shape
        stacks, cycle = w_cur.shape[:2]
        parts = n // batch
        srcs = n // parts
        rows, halves, reach = seq_dev * srcs, channels // LANES, 2 ** (cycle - 1)
        per = rows // n
        any_space = pl.BlockSpec(memory_space=pl.ANY)
        dma = pltpu.SemaphoreType.DMA
        out = pl.pallas_call(
            functools.partial(stack_kernel, n),
            out_shape=jax.ShapeDtypeStruct((batch, parts, 2, per, channels), F32),
            in_specs=[any_space] * 5,
            out_specs=any_space,
            scratch_shapes=[
                pltpu.VMEM((rows, channels), BF16),
                pltpu.VMEM((2, halves, reach + rows, LANES), F32),
                pltpu.VMEM((halves, rows, LANES), F32),
                pltpu.VMEM((2, 2) + w_cur.shape[1:], BF16),
                pltpu.VMEM((2, 2) + w_res.shape[1:], BF16),
                pltpu.VMEM((stacks, halves, 2 * reach, LANES), F32),
                pltpu.VMEM((stacks, halves, 2 * reach, LANES), F32),
                pltpu.VMEM((n, 2, per, channels), F32),
                dma((2, 4)), dma((batch,)), dma((srcs,)), dma((stacks,)), dma((stacks,)), dma((n,)), dma((n,)), dma,
            ],
            compiler_params=pltpu.CompilerParams(collective_id=0, has_side_effects=True, vmem_limit_bytes=56 << 20),
            name="conv_stack",
        )(x_loc, w_cur, w_past, w_res, w_skip)
        shape = (batch, 1, parts * per, channels)
        return out[:, :, 0].reshape(shape), out[:, :, 1].reshape(shape)

    return jax.shard_map(local_stack, mesh=mesh, in_specs=(P("dp", "sp", None), P(), P(), P(), P()), out_specs=(P("dp", "sp", None, None), P("dp", "sp", None, None)), check_vma=False)
```

```python
import functools
import math

import jax
import jax.numpy as jnp
from jax import lax
from jax.experimental import pallas as pl
from jax.experimental.pallas import tpu as pltpu
from jax.sharding import PartitionSpec as P

F32, BF16 = jnp.float32, jnp.bfloat16
LANES = 128
UNROLL = 2
VMEM = 50


def load_rows(ref, start, count):
    return jnp.concatenate([ref[g, pl.ds(start, count), :] for g in range(ref.shape[0])], axis=1)


def store_rows(ref, start, value):
    for g in range(ref.shape[0]):
        ref[g, pl.ds(start, value.shape[0]), :] = value[:, g * LANES:(g + 1) * LANES]


def gated(z):
    c = z.shape[1] // 2
    return (jnp.tanh(z[:, :c]) * (0.5 * jnp.tanh(0.5 * z[:, c:]) + 0.5)).astype(BF16)


def send_order(side, cores):
    def reach(v):
        return min(v, side - v)
    offsets = [(dx, dy, dc) for dc in range(cores) for dy in range(side) for dx in range(side)]
    return sorted(offsets, key=lambda o: -reach(o[0]) - reach(o[1]))


def stack_kernel(n, unroll, x_ref, wc, wp, wr, ws, out_ref, xv, xbuf, h, skip, win, wout, halo_out, halo_in, stage,
                 w_sem, x_send, x_recv, halo_send, halo_recv, o_send, o_recv, self_sem):
    me = lax.axis_index("sp")
    batch, seq_dev = x_ref.shape[0], x_ref.shape[1]
    parts = n // batch
    srcs = n // parts
    rows = seq_dev * srcs
    stacks, cycle = wc.shape[0], wc.shape[1]
    reach = 2 ** (cycle - 1)
    seq, part = me // parts, lax.rem(me, parts)
    my_part = me // srcs
    side = math.isqrt(batch)
    chip_y, chip_x = seq // side, lax.rem(seq, side)

    def chip_at(dx, dy):
        return lax.rem(chip_y + dy, side) * side + lax.rem(chip_x + dx, side)

    def weight_copies(s, slot):
        return [pltpu.make_async_copy(w.at[s], buf.at[slot, t], w_sem.at[slot, 2 * o + t])
                for o, (buf, pair) in enumerate(((win, (wc, wp)), (wout, (wr, ws)))) for t, w in enumerate(pair)]

    x_in = pltpu.make_async_copy(x_ref, xv, self_sem)
    x_in.start()
    for c in weight_copies(0, 0):
        c.start()
    halo_in[0] = jnp.zeros(halo_in.shape[1:], F32)
    skip[...] = jnp.zeros_like(skip)

    barrier = pltpu.get_barrier_semaphore()

    def greet(k, _):
        pl.semaphore_signal(barrier, inc=1, device_id={"sp": lax.rem(me + k, n)}, device_id_type=pl.DeviceIdType.MESH)
        return 0
    lax.fori_loop(1, n, greet, 0)
    x_in.wait()
    pl.semaphore_wait(barrier, n - 1)

    slot_x = pl.ds(lax.rem(me, srcs) * seq_dev, seq_dev)

    def x_copy(b):
        return pltpu.make_async_remote_copy(
            src_ref=xv.at[b], dst_ref=xbuf.at[slot_x], send_sem=x_send, recv_sem=x_recv,
            device_id={"sp": b * parts + my_part}, device_id_type=pl.DeviceIdType.MESH)

    def x_start(b):
        @pl.when(b * parts + my_part != me)
        def _():
            x_copy(b).start()

        @pl.when(b * parts + my_part == me)
        def _():
            pltpu.make_async_copy(x_ref.at[b], xbuf.at[slot_x], x_recv).start()
    for dx, dy, _ in send_order(side, 1):
        x_start(chip_at(dx, dy))

    pltpu.make_async_copy(xbuf, xbuf, x_recv).wait()
    store_rows(h.at[0], reach, xbuf[...].astype(F32))

    def layer(s, i, slot):
        src, dst = h.at[i % 2], h.at[(i + 1) % 2]
        d = 2 ** i
        for g in range(h.shape[1]):
            src[g, pl.ds(reach - d, d), :] = halo_in[s * part, g, pl.ds(d, d), :]
            halo_out[s, g, pl.ds(d, d), :] = src[g, pl.ds(reach + rows - d, d), :]
        cur = load_rows(src, reach, rows)
        past = load_rows(src, reach - d, rows).astype(BF16)
        z = (jnp.dot(cur.astype(BF16), win[slot, 0, i], preferred_element_type=F32)
             + jnp.dot(past, win[slot, 1, i], preferred_element_type=F32))
        a = gated(z)
        store_rows(dst, reach, cur + jnp.dot(a, wout[slot, 0, i], preferred_element_type=F32))
        store_rows(skip, 0, load_rows(skip, 0, rows) + jnp.dot(a, wout[slot, 1, i], preferred_element_type=F32))

    def halo_copy(s):
        return pltpu.make_async_remote_copy(
            src_ref=halo_out.at[s], dst_ref=halo_in.at[s], send_sem=halo_send, recv_sem=halo_recv.at[s],
            device_id={"sp": jnp.minimum(me + 1, n - 1)}, device_id_type=pl.DeviceIdType.MESH)

    def stack(s, slot):
        for c in weight_copies(s, slot):
            c.wait()

        @pl.when(s + 1 < stacks)
        def _():
            for c in weight_copies(s + 1, 1 - slot):
                c.start()

        @pl.when(part > 0)
        def _():
            halo_copy(s).wait_recv()
        for i in range(cycle):
            layer(s, i, slot)

        @pl.when(part < parts - 1)
        def _():
            halo_copy(s).start()

    def stack_group(q, _):
        for r in range(unroll):
            s = q * unroll + r
            stack(s, r % 2 if unroll % 2 == 0 else lax.rem(s, 2))
        return 0
    lax.fori_loop(0, stacks // unroll, stack_group, 0)

    per = rows // n
    for j in range(n):
        for g in range(h.shape[1]):
            stage[j, 0, :, g * LANES:(g + 1) * LANES] = h[0, g, pl.ds(reach + j, per, stride=n), :]
            stage[j, 1, :, g * LANES:(g + 1) * LANES] = skip[g, pl.ds(j, per, stride=n), :]

    def out_copy(target, source):
        return pltpu.make_async_remote_copy(
            src_ref=stage.at[target], dst_ref=out_ref.at[source // parts, lax.rem(source, parts)],
            send_sem=o_send, recv_sem=o_recv,
            device_id={"sp": target}, device_id_type=pl.DeviceIdType.MESH)

    for dx, dy, dc in send_order(side, parts):
        if (dx, dy, dc) != (0, 0, 0):
            out_copy(chip_at(dx, dy) * parts + lax.rem(part + dc, parts), me).start()
    pltpu.make_async_copy(stage.at[me], out_ref.at[seq, part], o_recv).start()

    blocks = batch - (my_part == part).astype(jnp.int32)
    for count in (batch - 1, batch):
        @pl.when(blocks == count)
        def _():
            pltpu.make_async_copy(xv.at[pl.ds(0, count)], xv.at[pl.ds(0, count)], x_send).wait()

    @pl.when(part < parts - 1)
    def _():
        pltpu.make_async_copy(halo_out, halo_out, halo_send).wait()
    pltpu.make_async_copy(stage.at[pl.ds(0, n - 1)], stage.at[pl.ds(0, n - 1)], o_send).wait()
    pltpu.make_async_copy(out_ref, out_ref, o_recv).wait()


def split_kernel(both_ref, h_ref, skip_ref, sem):
    copies = [pltpu.make_async_copy(both_ref.at[:, :, t], ref, sem.at[t]) for t, ref in enumerate((h_ref, skip_ref))]
    for c in copies:
        c.start()
    for c in copies:
        c.wait()


def solution(mesh):
    n = mesh.shape["sp"]

    def local_stack(x_loc, w_cur, w_past, w_res, w_skip):
        batch, seq_dev, channels = x_loc.shape
        stacks, cycle = w_cur.shape[:2]
        parts = n // batch
        srcs = n // parts
        rows, halves, reach = seq_dev * srcs, channels // LANES, 2 ** (cycle - 1)
        per = rows // n
        any_space = pl.BlockSpec(memory_space=pl.ANY)
        dma = pltpu.SemaphoreType.DMA
        out = pl.pallas_call(
            functools.partial(stack_kernel, n, UNROLL),
            out_shape=jax.ShapeDtypeStruct((batch, parts, 2, per, channels), F32),
            in_specs=[pl.BlockSpec(memory_space=pltpu.HBM)] * 5,
            out_specs=any_space,
            scratch_shapes=[
                pltpu.VMEM(x_loc.shape, BF16),
                pltpu.VMEM((rows, channels), BF16),
                pltpu.VMEM((2, halves, reach + rows, LANES), F32),
                pltpu.VMEM((halves, rows, LANES), F32),
                pltpu.VMEM((2, 2) + w_cur.shape[1:], BF16),
                pltpu.VMEM((2, 2) + w_res.shape[1:], BF16),
                pltpu.VMEM((stacks, halves, 2 * reach, LANES), F32),
                pltpu.VMEM((stacks, halves, 2 * reach, LANES), F32),
                pltpu.VMEM((n, 2, per, channels), F32),
                dma((2, 4)), dma, dma, dma, dma((stacks,)), dma, dma, dma,
            ],
            compiler_params=pltpu.CompilerParams(collective_id=0, has_side_effects=True, vmem_limit_bytes=VMEM << 20),
            name="conv_stack",
        )(pltpu.with_memory_space_constraint(x_loc, pltpu.HBM), w_cur, w_past, w_res, w_skip)
        shape = (batch, 1, parts * per, channels)
        one = jax.ShapeDtypeStruct((batch, parts, per, channels), F32)
        h_out, skip_out = pl.pallas_call(
            split_kernel,
            out_shape=[one, one],
            in_specs=[any_space], out_specs=[any_space] * 2,
            scratch_shapes=[dma((2,))],
            compiler_params=pltpu.CompilerParams(vmem_limit_bytes=VMEM << 20),
            name="split",
        )(out)
        return h_out.reshape(shape), skip_out.reshape(shape)

    return jax.shard_map(local_stack, mesh=mesh, in_specs=(P("dp", "sp", None), P(), P(), P(), P()), out_specs=(P("dp", "sp", None, None), P("dp", "sp", None, None)), check_vma=False)
```

```python
import functools
import math

import jax
import jax.numpy as jnp
from jax import lax
from jax.experimental import pallas as pl
from jax.experimental.pallas import tpu as pltpu
from jax.sharding import PartitionSpec as P

F32, BF16 = jnp.float32, jnp.bfloat16
LANES = 128
SUBLANES = 8
UNROLL = 2
VMEM = 50


def load_rows(ref, start, count):
    return jnp.concatenate([ref[g, pl.ds(start, count), :] for g in range(ref.shape[0])], axis=1)


def store_rows(ref, start, value):
    for g in range(ref.shape[0]):
        ref[g, pl.ds(start, value.shape[0]), :] = value[:, g * LANES:(g + 1) * LANES]


def gated(z):
    c = z.shape[1] // 2
    return (jnp.tanh(z[:, :c]) * (0.5 * jnp.tanh(0.5 * z[:, c:]) + 0.5)).astype(BF16)


def send_order(side, cores):
    def reach(v):
        return min(v, side - v)
    offsets = [(dx, dy, dc) for dc in range(cores) for dy in range(side) for dx in range(side)]
    return sorted(offsets, key=lambda o: -reach(o[0]) - reach(o[1]))


def stack_kernel(n, unroll, x_ref, wc, wp, wr, ws, out_ref, xv, xbuf, h, skip, win, wout, halo_out, halo_in, stage,
                 w_sem, x_send, x_recv, halo_send, halo_recv, o_send, o_recv, self_sem):
    me = lax.axis_index("sp")
    batch, seq_dev = x_ref.shape[0], x_ref.shape[1]
    parts = n // batch
    srcs = n // parts
    rows = seq_dev * srcs
    stacks, cycle = wc.shape[0], wc.shape[1]
    reach = 2 ** (cycle - 1)
    seq, part = me // parts, lax.rem(me, parts)
    my_part = me // srcs
    side = math.isqrt(batch)
    chip_y, chip_x = seq // side, lax.rem(seq, side)

    def chip_at(dx, dy):
        return lax.rem(chip_y + dy, side) * side + lax.rem(chip_x + dx, side)

    def weight_copies(s, slot):
        return [pltpu.make_async_copy(w.at[s], buf.at[slot, t], w_sem.at[slot, 2 * o + t])
                for o, (buf, pair) in enumerate(((win, (wc, wp)), (wout, (wr, ws)))) for t, w in enumerate(pair)]

    x_in = pltpu.make_async_copy(x_ref, xv, self_sem)
    x_in.start()
    for c in weight_copies(0, 0):
        c.start()
    halo_in[0] = jnp.zeros(halo_in.shape[1:], F32)
    skip[...] = jnp.zeros_like(skip)

    barrier = pltpu.get_barrier_semaphore()

    def greet(k, _):
        pl.semaphore_signal(barrier, inc=1, device_id={"sp": lax.rem(me + k, n)}, device_id_type=pl.DeviceIdType.MESH)
        return 0
    lax.fori_loop(1, n, greet, 0)
    x_in.wait()
    pl.semaphore_wait(barrier, n - 1)

    slot_x = pl.ds(lax.rem(me, srcs) * seq_dev, seq_dev)

    def x_copy(b):
        return pltpu.make_async_remote_copy(
            src_ref=xv.at[b], dst_ref=xbuf.at[slot_x], send_sem=x_send, recv_sem=x_recv,
            device_id={"sp": b * parts + my_part}, device_id_type=pl.DeviceIdType.MESH)

    def x_start(b):
        @pl.when(b * parts + my_part != me)
        def _():
            x_copy(b).start()

        @pl.when(b * parts + my_part == me)
        def _():
            pltpu.make_async_copy(x_ref.at[b], xbuf.at[slot_x], x_recv).start()
    for dx, dy, _ in send_order(side, 1):
        x_start(chip_at(dx, dy))

    pltpu.make_async_copy(xbuf, xbuf, x_recv).wait()
    store_rows(h.at[0], reach, xbuf[...].astype(F32))

    def layer(s, i, slot):
        src, dst = h.at[i % 2], h.at[(i + 1) % 2]
        d = 2 ** i
        for g in range(h.shape[1]):
            src[g, pl.ds(reach - d, d), :] = halo_in[s * part, g, pl.ds(d, d), :]
            halo_out[s, g, pl.ds(d, d), :] = src[g, pl.ds(reach + rows - d, d), :]
        cur = load_rows(src, reach, rows)
        if d < SUBLANES:
            past = pltpu.roll(jnp.concatenate([load_rows(src, reach - SUBLANES, SUBLANES), cur], axis=0), d, 0)[SUBLANES:]
        else:
            past = load_rows(src, reach - d, rows)
        past = past.astype(BF16)
        z = (jnp.dot(cur.astype(BF16), win[slot, 0, i], preferred_element_type=F32)
             + jnp.dot(past, win[slot, 1, i], preferred_element_type=F32))
        a = gated(z)
        store_rows(dst, reach, cur + jnp.dot(a, wout[slot, 0, i], preferred_element_type=F32))
        store_rows(skip, 0, load_rows(skip, 0, rows) + jnp.dot(a, wout[slot, 1, i], preferred_element_type=F32))

    def halo_copy(s):
        return pltpu.make_async_remote_copy(
            src_ref=halo_out.at[s], dst_ref=halo_in.at[s], send_sem=halo_send, recv_sem=halo_recv.at[s],
            device_id={"sp": jnp.minimum(me + 1, n - 1)}, device_id_type=pl.DeviceIdType.MESH)

    def stack(s, slot):
        for c in weight_copies(s, slot):
            c.wait()

        @pl.when(s + 1 < stacks)
        def _():
            for c in weight_copies(s + 1, 1 - slot):
                c.start()

        @pl.when(part > 0)
        def _():
            halo_copy(s).wait_recv()
        for i in range(cycle):
            layer(s, i, slot)

        @pl.when(part < parts - 1)
        def _():
            halo_copy(s).start()

    def stack_group(q, _):
        for r in range(unroll):
            s = q * unroll + r
            stack(s, r % 2 if unroll % 2 == 0 else lax.rem(s, 2))
        return 0
    lax.fori_loop(0, stacks // unroll, stack_group, 0)

    per = rows // n
    for j in range(n):
        for g in range(h.shape[1]):
            stage[j, 0, :, g * LANES:(g + 1) * LANES] = h[0, g, pl.ds(reach + j, per, stride=n), :]
            stage[j, 1, :, g * LANES:(g + 1) * LANES] = skip[g, pl.ds(j, per, stride=n), :]

    def out_copy(target, source):
        return pltpu.make_async_remote_copy(
            src_ref=stage.at[target], dst_ref=out_ref.at[source // parts, lax.rem(source, parts)],
            send_sem=o_send, recv_sem=o_recv,
            device_id={"sp": target}, device_id_type=pl.DeviceIdType.MESH)

    for dx, dy, dc in send_order(side, parts):
        if (dx, dy, dc) != (0, 0, 0):
            out_copy(chip_at(dx, dy) * parts + lax.rem(part + dc, parts), me).start()
    pltpu.make_async_copy(stage.at[me], out_ref.at[seq, part], o_recv).start()

    blocks = batch - (my_part == part).astype(jnp.int32)
    for count in (batch - 1, batch):
        @pl.when(blocks == count)
        def _():
            pltpu.make_async_copy(xv.at[pl.ds(0, count)], xv.at[pl.ds(0, count)], x_send).wait()

    @pl.when(part < parts - 1)
    def _():
        pltpu.make_async_copy(halo_out, halo_out, halo_send).wait()
    pltpu.make_async_copy(stage.at[pl.ds(0, n - 1)], stage.at[pl.ds(0, n - 1)], o_send).wait()
    pltpu.make_async_copy(out_ref, out_ref, o_recv).wait()


def split_kernel(both_ref, h_ref, skip_ref, sem):
    copies = [pltpu.make_async_copy(both_ref.at[:, :, t], ref, sem.at[t]) for t, ref in enumerate((h_ref, skip_ref))]
    for c in copies:
        c.start()
    for c in copies:
        c.wait()


def solution(mesh):
    n = mesh.shape["sp"]

    def local_stack(x_loc, w_cur, w_past, w_res, w_skip):
        batch, seq_dev, channels = x_loc.shape
        stacks, cycle = w_cur.shape[:2]
        parts = n // batch
        srcs = n // parts
        rows, halves, reach = seq_dev * srcs, channels // LANES, 2 ** (cycle - 1)
        per = rows // n
        any_space = pl.BlockSpec(memory_space=pl.ANY)
        dma = pltpu.SemaphoreType.DMA
        out = pl.pallas_call(
            functools.partial(stack_kernel, n, UNROLL),
            out_shape=jax.ShapeDtypeStruct((batch, parts, 2, per, channels), F32),
            in_specs=[pl.BlockSpec(memory_space=pltpu.HBM)] * 5,
            out_specs=any_space,
            scratch_shapes=[
                pltpu.VMEM(x_loc.shape, BF16),
                pltpu.VMEM((rows, channels), BF16),
                pltpu.VMEM((2, halves, reach + rows, LANES), F32),
                pltpu.VMEM((halves, rows, LANES), F32),
                pltpu.VMEM((2, 2) + w_cur.shape[1:], BF16),
                pltpu.VMEM((2, 2) + w_res.shape[1:], BF16),
                pltpu.VMEM((stacks, halves, 2 * reach, LANES), F32),
                pltpu.VMEM((stacks, halves, 2 * reach, LANES), F32),
                pltpu.VMEM((n, 2, per, channels), F32),
                dma((2, 4)), dma, dma, dma, dma((stacks,)), dma, dma, dma,
            ],
            compiler_params=pltpu.CompilerParams(collective_id=0, has_side_effects=True, vmem_limit_bytes=VMEM << 20),
            name="conv_stack",
        )(pltpu.with_memory_space_constraint(x_loc, pltpu.HBM), w_cur, w_past, w_res, w_skip)
        shape = (batch, 1, parts * per, channels)
        one = jax.ShapeDtypeStruct((batch, parts, per, channels), F32)
        h_out, skip_out = pl.pallas_call(
            split_kernel,
            out_shape=[one, one],
            in_specs=[any_space], out_specs=[any_space] * 2,
            scratch_shapes=[dma((2,))],
            compiler_params=pltpu.CompilerParams(vmem_limit_bytes=VMEM << 20),
            name="split",
        )(out)
        return h_out.reshape(shape), skip_out.reshape(shape)

    return jax.shard_map(local_stack, mesh=mesh, in_specs=(P("dp", "sp", None), P(), P(), P(), P()), out_specs=(P("dp", "sp", None, None), P("dp", "sp", None, None)), check_vma=False)
```

```python
import functools
import math

import jax
import jax.numpy as jnp
from jax import lax
from jax.experimental import pallas as pl
from jax.experimental.pallas import tpu as pltpu
from jax.sharding import PartitionSpec as P

F32, BF16 = jnp.float32, jnp.bfloat16
LANES = 128
SUBLANES = 8
UNROLL = 2
VMEM = 50


def load_rows(ref, start, count):
    return jnp.concatenate([ref[g, pl.ds(start, count), :] for g in range(ref.shape[0])], axis=1)


def store_rows(ref, start, value):
    for g in range(ref.shape[0]):
        ref[g, pl.ds(start, value.shape[0]), :] = value[:, g * LANES:(g + 1) * LANES]


def gated(z):
    c = z.shape[1] // 2
    return (jnp.tanh(z[:, :c]) * (0.5 * jnp.tanh(0.5 * z[:, c:]) + 0.5)).astype(BF16)


def send_order(side, cores):
    def reach(v):
        return min(v, side - v)
    offsets = [(dx, dy, dc) for dc in range(cores) for dy in range(side) for dx in range(side)]
    return sorted(offsets, key=lambda o: -reach(o[0]) - reach(o[1]))


def stack_kernel(n, unroll, x_ref, wc, wp, wr, ws, out_ref, xv, xbuf, h, skip, win, wout, halo_out, halo_in, stage,
                 w_sem, x_send, x_recv, halo_send, halo_recv, o_send, o_recv, self_sem):
    me = lax.axis_index("sp")
    batch, seq_dev = x_ref.shape[0], x_ref.shape[1]
    parts = n // batch
    srcs = n // parts
    rows = seq_dev * srcs
    stacks, cycle = wc.shape[0], wc.shape[1]
    reach = 2 ** (cycle - 1)
    seq, part = me // parts, lax.rem(me, parts)
    my_part = me // srcs
    side = math.isqrt(batch)
    chip_y, chip_x = seq // side, lax.rem(seq, side)

    def chip_at(dx, dy):
        return lax.rem(chip_y + dy, side) * side + lax.rem(chip_x + dx, side)

    def weight_copies(s, slot):
        return [pltpu.make_async_copy(w.at[s], buf.at[slot, t], w_sem.at[slot, 2 * o + t])
                for o, (buf, pair) in enumerate(((win, (wc, wp)), (wout, (wr, ws)))) for t, w in enumerate(pair)]

    x_in = pltpu.make_async_copy(x_ref, xv, self_sem)
    x_in.start()
    for c in weight_copies(0, 0):
        c.start()
    halo_in[0] = jnp.zeros(halo_in.shape[1:], F32)
    skip[...] = jnp.zeros_like(skip)

    barrier = pltpu.get_barrier_semaphore()

    def greet(k, _):
        pl.semaphore_signal(barrier, inc=1, device_id={"sp": lax.rem(me + k, n)}, device_id_type=pl.DeviceIdType.MESH)
        return 0
    lax.fori_loop(1, n, greet, 0)
    x_in.wait()
    pl.semaphore_wait(barrier, n - 1)

    slot_x = pl.ds(lax.rem(me, srcs) * seq_dev, seq_dev)

    def x_copy(b):
        return pltpu.make_async_remote_copy(
            src_ref=xv.at[b], dst_ref=xbuf.at[slot_x], send_sem=x_send, recv_sem=x_recv,
            device_id={"sp": b * parts + my_part}, device_id_type=pl.DeviceIdType.MESH)

    for dx, dy, _ in send_order(side, 1):
        if (dx, dy) != (0, 0):
            x_copy(chip_at(dx, dy)).start()

    @pl.when(my_part != part)
    def _():
        x_copy(seq).start()

    @pl.when(my_part == part)
    def _():
        pltpu.make_async_copy(x_ref.at[seq], xbuf.at[slot_x], x_recv).start()
    pltpu.make_async_copy(xbuf, xbuf, x_recv).wait()
    store_rows(h.at[0], reach, xbuf[...].astype(F32))

    def layer(s, i, slot):
        src, dst = h.at[i % 2], h.at[(i + 1) % 2]
        d = 2 ** i
        for g in range(h.shape[1]):
            src[g, pl.ds(reach - d, d), :] = halo_in[s * part, g, pl.ds(d, d), :]
            halo_out[s, g, pl.ds(d, d), :] = src[g, pl.ds(reach + rows - d, d), :]
        cur = load_rows(src, reach, rows)
        if d < SUBLANES:
            past = pltpu.roll(jnp.concatenate([load_rows(src, reach - SUBLANES, SUBLANES), cur], axis=0), d, 0)[SUBLANES:]
        else:
            past = load_rows(src, reach - d, rows)
        past = past.astype(BF16)
        z = (jnp.dot(cur.astype(BF16), win[slot, 0, i], preferred_element_type=F32)
             + jnp.dot(past, win[slot, 1, i], preferred_element_type=F32))
        a = gated(z)
        store_rows(dst, reach, cur + jnp.dot(a, wout[slot, 0, i], preferred_element_type=F32))
        store_rows(skip, 0, load_rows(skip, 0, rows) + jnp.dot(a, wout[slot, 1, i], preferred_element_type=F32))

    def halo_copy(s):
        return pltpu.make_async_remote_copy(
            src_ref=halo_out.at[s], dst_ref=halo_in.at[s], send_sem=halo_send, recv_sem=halo_recv.at[s],
            device_id={"sp": jnp.minimum(me + 1, n - 1)}, device_id_type=pl.DeviceIdType.MESH)

    def stack(s, slot):
        for c in weight_copies(s, slot):
            c.wait()

        @pl.when(s + 1 < stacks)
        def _():
            for c in weight_copies(s + 1, 1 - slot):
                c.start()

        @pl.when(part > 0)
        def _():
            halo_copy(s).wait_recv()
        for i in range(cycle):
            layer(s, i, slot)

        @pl.when(part < parts - 1)
        def _():
            halo_copy(s).start()

    def stack_group(q, _):
        for r in range(unroll):
            s = q * unroll + r
            stack(s, r % 2 if unroll % 2 == 0 else lax.rem(s, 2))
        return 0
    lax.fori_loop(0, stacks // unroll, stack_group, 0)

    per = rows // n
    for t, (state, first) in enumerate(((h.at[0], reach), (skip, 0))):
        for g in range(h.shape[1]):
            by_turn = state[g, pl.ds(first, rows), :].reshape(per, n, LANES)
            stage[:, t, :, g * LANES:(g + 1) * LANES] = jnp.swapaxes(by_turn, 0, 1)

    def out_copy(target, source):
        return pltpu.make_async_remote_copy(
            src_ref=stage.at[target], dst_ref=out_ref.at[source // parts, lax.rem(source, parts)],
            send_sem=o_send, recv_sem=o_recv,
            device_id={"sp": target}, device_id_type=pl.DeviceIdType.MESH)

    for dx, dy, dc in send_order(side, parts):
        if (dx, dy, dc) != (0, 0, 0):
            out_copy(chip_at(dx, dy) * parts + lax.rem(part + dc, parts), me).start()
    pltpu.make_async_copy(stage.at[me], out_ref.at[seq, part], o_recv).start()

    blocks = batch - (my_part == part).astype(jnp.int32)
    for count in (batch - 1, batch):
        @pl.when(blocks == count)
        def _():
            pltpu.make_async_copy(xv.at[pl.ds(0, count)], xv.at[pl.ds(0, count)], x_send).wait()

    @pl.when(part < parts - 1)
    def _():
        pltpu.make_async_copy(halo_out, halo_out, halo_send).wait()
    pltpu.make_async_copy(stage.at[pl.ds(0, n - 1)], stage.at[pl.ds(0, n - 1)], o_send).wait()
    pltpu.make_async_copy(out_ref, out_ref, o_recv).wait()


def split_kernel(both_ref, h_ref, skip_ref, sem):
    copies = [pltpu.make_async_copy(both_ref.at[:, :, t], ref, sem.at[t]) for t, ref in enumerate((h_ref, skip_ref))]
    for c in copies:
        c.start()
    for c in copies:
        c.wait()


def solution(mesh):
    n = mesh.shape["sp"]

    def local_stack(x_loc, w_cur, w_past, w_res, w_skip):
        batch, seq_dev, channels = x_loc.shape
        stacks, cycle = w_cur.shape[:2]
        parts = n // batch
        srcs = n // parts
        rows, halves, reach = seq_dev * srcs, channels // LANES, 2 ** (cycle - 1)
        per = rows // n
        any_space = pl.BlockSpec(memory_space=pl.ANY)
        dma = pltpu.SemaphoreType.DMA
        out = pl.pallas_call(
            functools.partial(stack_kernel, n, UNROLL),
            out_shape=jax.ShapeDtypeStruct((batch, parts, 2, per, channels), F32),
            in_specs=[pl.BlockSpec(memory_space=pltpu.HBM)] * 5,
            out_specs=any_space,
            scratch_shapes=[
                pltpu.VMEM(x_loc.shape, BF16),
                pltpu.VMEM((rows, channels), BF16),
                pltpu.VMEM((2, halves, reach + rows, LANES), F32),
                pltpu.VMEM((halves, rows, LANES), F32),
                pltpu.VMEM((2, 2) + w_cur.shape[1:], BF16),
                pltpu.VMEM((2, 2) + w_res.shape[1:], BF16),
                pltpu.VMEM((stacks, halves, 2 * reach, LANES), F32),
                pltpu.VMEM((stacks, halves, 2 * reach, LANES), F32),
                pltpu.VMEM((n, 2, per, channels), F32),
                dma((2, 4)), dma, dma, dma, dma((stacks,)), dma, dma, dma,
            ],
            compiler_params=pltpu.CompilerParams(collective_id=0, has_side_effects=True, vmem_limit_bytes=VMEM << 20),
            name="conv_stack",
        )(pltpu.with_memory_space_constraint(x_loc, pltpu.HBM), w_cur, w_past, w_res, w_skip)
        shape = (batch, 1, parts * per, channels)
        one = jax.ShapeDtypeStruct((batch, parts, per, channels), F32)
        h_out, skip_out = pl.pallas_call(
            split_kernel,
            out_shape=[one, one],
            in_specs=[any_space], out_specs=[any_space] * 2,
            scratch_shapes=[dma((2,))],
            compiler_params=pltpu.CompilerParams(vmem_limit_bytes=VMEM << 20),
            name="split",
        )(out)
        return h_out.reshape(shape), skip_out.reshape(shape)

    return jax.shard_map(local_stack, mesh=mesh, in_specs=(P("dp", "sp", None), P(), P(), P(), P()), out_specs=(P("dp", "sp", None, None), P("dp", "sp", None, None)), check_vma=False)
```

```python
import functools
import math

import jax
import jax.numpy as jnp
from jax import lax
from jax.experimental import pallas as pl
from jax.experimental.pallas import tpu as pltpu
from jax.sharding import PartitionSpec as P

F32, BF16 = jnp.float32, jnp.bfloat16
LANES = 128
SUBLANES = 8
UNROLL = 2
VMEM = 50


def load_rows(ref, start, count):
    return jnp.concatenate([ref[g, pl.ds(start, count), :] for g in range(ref.shape[0])], axis=1)


def store_rows(ref, start, value):
    for g in range(ref.shape[0]):
        ref[g, pl.ds(start, value.shape[0]), :] = value[:, g * LANES:(g + 1) * LANES]


def gated(z):
    c = z.shape[1] // 2
    return (jnp.tanh(z[:, :c]) * (0.5 * jnp.tanh(0.5 * z[:, c:]) + 0.5)).astype(BF16)


def send_order(side, cores):
    def reach(v):
        return min(v, side - v)
    offsets = [(dx, dy, dc) for dc in range(cores) for dy in range(side) for dx in range(side)]
    return sorted(offsets, key=lambda o: -reach(o[0]) - reach(o[1]))


def stack_kernel(n, unroll, x_ref, wc, wp, wr, ws, out_ref, xv, xbuf, h, skip, win, wout, halo_out, halo_in, stage,
                 w_sem, x_send, x_recv, halo_send, halo_recv, o_send, o_recv, self_sem):
    me = lax.axis_index("sp")
    batch, seq_dev = x_ref.shape[0], x_ref.shape[1]
    parts = n // batch
    srcs = n // parts
    rows = seq_dev * srcs
    stacks, cycle = wc.shape[0], wc.shape[1]
    reach = 2 ** (cycle - 1)
    seq, part = me // parts, lax.rem(me, parts)
    my_part = me // srcs
    side = math.isqrt(batch)
    chip_y, chip_x = seq // side, lax.rem(seq, side)

    def chip_at(dx, dy):
        return lax.rem(chip_y + dy, side) * side + lax.rem(chip_x + dx, side)

    def weight_copies(s, slot):
        return [pltpu.make_async_copy(w.at[s], buf.at[slot, t], w_sem.at[slot, o])
                for o, (buf, pair) in enumerate(((win, (wc, wp)), (wout, (wr, ws)))) for t, w in enumerate(pair)]

    x_in = pltpu.make_async_copy(x_ref, xv, self_sem)
    x_in.start()
    for c in weight_copies(0, 0):
        c.start()
    halo_in[0] = jnp.zeros(halo_in.shape[1:], F32)
    skip[...] = jnp.zeros_like(skip)

    barrier = pltpu.get_barrier_semaphore()

    def greet(k, _):
        pl.semaphore_signal(barrier, inc=1, device_id={"sp": lax.rem(me + k, n)}, device_id_type=pl.DeviceIdType.MESH)
        return 0
    lax.fori_loop(1, n, greet, 0)
    x_in.wait()
    pl.semaphore_wait(barrier, n - 1)

    slot_x = pl.ds(lax.rem(me, srcs) * seq_dev, seq_dev)

    def x_copy(b):
        return pltpu.make_async_remote_copy(
            src_ref=xv.at[b], dst_ref=xbuf.at[slot_x], send_sem=x_send, recv_sem=x_recv,
            device_id={"sp": b * parts + my_part}, device_id_type=pl.DeviceIdType.MESH)

    for dx, dy, _ in send_order(side, 1):
        if (dx, dy) != (0, 0):
            x_copy(chip_at(dx, dy)).start()

    @pl.when(my_part != part)
    def _():
        x_copy(seq).start()

    @pl.when(my_part == part)
    def _():
        pltpu.make_async_copy(x_ref.at[seq], xbuf.at[slot_x], x_recv).start()
    pltpu.make_async_copy(xbuf, xbuf, x_recv).wait()
    store_rows(h.at[0], reach, xbuf[...].astype(F32))

    def layer(s, i, slot):
        src, dst = h.at[i % 2], h.at[(i + 1) % 2]
        d = 2 ** i
        for g in range(h.shape[1]):
            src[g, pl.ds(reach - d, d), :] = halo_in[s * part, g, pl.ds(d, d), :]
            halo_out[s, g, pl.ds(d, d), :] = src[g, pl.ds(reach + rows - d, d), :]
        cur = load_rows(src, reach, rows)
        if d < SUBLANES:
            past = pltpu.roll(jnp.concatenate([load_rows(src, reach - SUBLANES, SUBLANES), cur], axis=0), d, 0)[SUBLANES:]
        else:
            past = load_rows(src, reach - d, rows)
        past = past.astype(BF16)
        z = (jnp.dot(cur.astype(BF16), win[slot, 0, i], preferred_element_type=F32)
             + jnp.dot(past, win[slot, 1, i], preferred_element_type=F32))
        a = gated(z)
        store_rows(dst, reach, cur + jnp.dot(a, wout[slot, 0, i], preferred_element_type=F32))
        store_rows(skip, 0, load_rows(skip, 0, rows) + jnp.dot(a, wout[slot, 1, i], preferred_element_type=F32))

    def halo_copy(s):
        return pltpu.make_async_remote_copy(
            src_ref=halo_out.at[s], dst_ref=halo_in.at[s], send_sem=halo_send, recv_sem=halo_recv.at[s],
            device_id={"sp": jnp.minimum(me + 1, n - 1)}, device_id_type=pl.DeviceIdType.MESH)

    def stack(s, slot):
        for o, buf in enumerate((win, wout)):
            pltpu.make_async_copy(buf.at[slot], buf.at[slot], w_sem.at[slot, o]).wait()

        @pl.when(s + 1 < stacks)
        def _():
            for c in weight_copies(s + 1, 1 - slot):
                c.start()

        @pl.when(part > 0)
        def _():
            halo_copy(s).wait_recv()
        for i in range(cycle):
            layer(s, i, slot)

        @pl.when(part < parts - 1)
        def _():
            halo_copy(s).start()

    def stack_group(q, _):
        for r in range(unroll):
            s = q * unroll + r
            stack(s, r % 2 if unroll % 2 == 0 else lax.rem(s, 2))
        return 0
    lax.fori_loop(0, stacks // unroll, stack_group, 0)

    per = rows // n
    for t, (state, first) in enumerate(((h.at[0], reach), (skip, 0))):
        for g in range(h.shape[1]):
            by_turn = state[g, pl.ds(first, rows), :].reshape(per, n, LANES)
            stage[:, t, :, g * LANES:(g + 1) * LANES] = jnp.swapaxes(by_turn, 0, 1)

    def out_copy(target, source):
        return pltpu.make_async_remote_copy(
            src_ref=stage.at[target], dst_ref=out_ref.at[source // parts, lax.rem(source, parts)],
            send_sem=o_send, recv_sem=o_recv,
            device_id={"sp": target}, device_id_type=pl.DeviceIdType.MESH)

    for dx, dy, dc in send_order(side, parts):
        if (dx, dy, dc) != (0, 0, 0):
            out_copy(chip_at(dx, dy) * parts + lax.rem(part + dc, parts), me).start()
    pltpu.make_async_copy(stage.at[me], out_ref.at[seq, part], o_recv).start()

    blocks = batch - (my_part == part).astype(jnp.int32)
    for count in (batch - 1, batch):
        @pl.when(blocks == count)
        def _():
            pltpu.make_async_copy(xv.at[pl.ds(0, count)], xv.at[pl.ds(0, count)], x_send).wait()

    @pl.when(part < parts - 1)
    def _():
        pltpu.make_async_copy(halo_out, halo_out, halo_send).wait()
    pltpu.make_async_copy(stage.at[pl.ds(0, n - 1)], stage.at[pl.ds(0, n - 1)], o_send).wait()
    pltpu.make_async_copy(out_ref, out_ref, o_recv).wait()


def split_kernel(both_ref, h_ref, skip_ref, sem):
    copies = [pltpu.make_async_copy(both_ref.at[:, :, t], ref, sem.at[t]) for t, ref in enumerate((h_ref, skip_ref))]
    for c in copies:
        c.start()
    for c in copies:
        c.wait()


def solution(mesh):
    n = mesh.shape["sp"]

    def local_stack(x_loc, w_cur, w_past, w_res, w_skip):
        batch, seq_dev, channels = x_loc.shape
        stacks, cycle = w_cur.shape[:2]
        parts = n // batch
        srcs = n // parts
        rows, halves, reach = seq_dev * srcs, channels // LANES, 2 ** (cycle - 1)
        per = rows // n
        any_space = pl.BlockSpec(memory_space=pl.ANY)
        dma = pltpu.SemaphoreType.DMA
        out = pl.pallas_call(
            functools.partial(stack_kernel, n, UNROLL),
            out_shape=jax.ShapeDtypeStruct((batch, parts, 2, per, channels), F32),
            in_specs=[pl.BlockSpec(memory_space=pltpu.HBM)] * 5,
            out_specs=any_space,
            scratch_shapes=[
                pltpu.VMEM(x_loc.shape, BF16),
                pltpu.VMEM((rows, channels), BF16),
                pltpu.VMEM((2, halves, reach + rows, LANES), F32),
                pltpu.VMEM((halves, rows, LANES), F32),
                pltpu.VMEM((2, 2) + w_cur.shape[1:], BF16),
                pltpu.VMEM((2, 2) + w_res.shape[1:], BF16),
                pltpu.VMEM((stacks, halves, 2 * reach, LANES), F32),
                pltpu.VMEM((stacks, halves, 2 * reach, LANES), F32),
                pltpu.VMEM((n, 2, per, channels), F32),
                dma((2, 2)), dma, dma, dma, dma((stacks,)), dma, dma, dma,
            ],
            compiler_params=pltpu.CompilerParams(collective_id=0, has_side_effects=True, vmem_limit_bytes=VMEM << 20),
            name="conv_stack",
        )(pltpu.with_memory_space_constraint(x_loc, pltpu.HBM), w_cur, w_past, w_res, w_skip)
        shape = (batch, 1, parts * per, channels)
        one = jax.ShapeDtypeStruct((batch, parts, per, channels), F32)
        h_out, skip_out = pl.pallas_call(
            split_kernel,
            out_shape=[one, one],
            in_specs=[any_space], out_specs=[any_space] * 2,
            scratch_shapes=[dma((2,))],
            compiler_params=pltpu.CompilerParams(vmem_limit_bytes=VMEM << 20),
            name="split",
        )(out)
        return h_out.reshape(shape), skip_out.reshape(shape)

    return jax.shard_map(local_stack, mesh=mesh, in_specs=(P("dp", "sp", None), P(), P(), P(), P()), out_specs=(P("dp", "sp", None, None), P("dp", "sp", None, None)), check_vma=False)
```
